16 devices in a mesh: rep: 1, dp: 16 (over x, y, z, core).
Axes of the slice: x: 2, y: 2, z: 2, core: 2. Of those that a mesh axis runs over, the one named last changes fastest.
Arguments:
- x: bfloat16 [16, 2048, 512], P(('rep', 'dp'))
- dy: bfloat16 [16, 2048, 512], P(('rep', 'dp'))
- w_gate: bfloat16 [2, 512, 8192], replicated
- w_up: bfloat16 [2, 512, 8192], replicated
- w_down: bfloat16 [2, 8192, 512], replicated
- m_w_gate: float32 [2, 512, 8192], P(None, 'dp')
- m_w_up: float32 [2, 512, 8192], P(None, 'dp')
- m_w_down: float32 [2, 8192, 512], P(None, 'dp')
- v_w_gate: float32 [2, 512, 8192], P(None, 'dp')
- v_w_up: float32 [2, 512, 8192], P(None, 'dp')
- v_w_down: float32 [2, 8192, 512], P(None, 'dp')
Outputs:
- output 1: bfloat16 [2, 512, 8192], P('rep')
- output 2: bfloat16 [2, 512, 8192], P('rep')
- output 3: bfloat16 [2, 8192, 512], P('rep')
- output 4: float32 [2, 512, 8192], P('rep', 'dp')
- output 5: float32 [2, 512, 8192], P('rep', 'dp')
- output 6: float32 [2, 8192, 512], P('rep', 'dp')
- output 7: float32 [2, 512, 8192], P('rep', 'dp')
- output 8: float32 [2, 512, 8192], P('rep', 'dp')
- output 9: float32 [2, 8192, 512], P('rep', 'dp')
All inputs are finite; a program needn't handle non-finite values.
Results may differ from the reference program's by a relative error of at most 0.022.
Values are sent between devices in bfloat16 or wider.
A program may use at most 2 GiB of HBM per device.

```python
import jax
import jax.numpy as jnp
from jax import lax

SEQUENCES = 16
TOKENS = 2048
D = 512
FF = 8192
LAYERS = 2
NAMES = ("w_gate", "w_up", "w_down")
SHAPES = {"w_gate": (LAYERS, D, FF), "w_up": (LAYERS, D, FF), "w_down": (LAYERS, FF, D)}


def bump(key, n, height):
    away = (jnp.arange(n, dtype=jnp.int32) - jax.random.randint(key, (), 0, n, jnp.int32)) % n
    return jnp.where(away < n // 8, height, 1.0)


def together(key, own, strength):
    shared = jax.random.normal(key, own.shape[1:], jnp.float32)
    return (own + strength * shared) * lax.rsqrt(1 + strength * strength)


def setup_inputs(seed: int = 0, part: int = 0) -> dict:
    kx, kdy, ka, kb, kz, kf, kh, kl, *keys = jax.random.split(jax.random.key(seed), 8 + 3 * len(NAMES))
    kx, kdy, ka, kb = (jax.random.fold_in(k, part) for k in (kx, kdy, ka, kb))
    kw, km, kv = (keys[i::3] for i in range(3))
    shape = (SEQUENCES, TOKENS, D)
    much_x, much_dy = jax.random.uniform(kz, (2,), jnp.float32, 0.0, 1.0)
    loud = 2.0 ** jax.random.uniform(jax.random.fold_in(kz, 1), (), jnp.float32, -1.0, 2.0)
    layers = 2.0 ** jax.random.uniform(kl, (LAYERS, 1, 1), jnp.float32, -1.0, 1.0)
    x = together(ka, jax.random.normal(kx, shape, jnp.float32), much_x) * bump(kf, D, 4.0)
    dy = together(kb, jax.random.normal(kdy, shape, jnp.float32), much_dy)
    drawn = {"x": x.astype(jnp.bfloat16), "dy": (loud * dy * (SEQUENCES * TOKENS) ** -0.5).astype(jnp.bfloat16)}
    for key, name in zip(kw, NAMES, strict=True):
        w = jax.random.normal(key, SHAPES[name], jnp.float32) * SHAPES[name][1] ** -0.5
        drawn[name] = (w * {"w_gate": 1.0, "w_up": bump(kh, FF, 4.0), "w_down": layers}[name]).astype(jnp.bfloat16)
    for key, name in zip(km, NAMES, strict=True):
        drawn[f"m_{name}"] = 0.1 * jax.random.normal(key, SHAPES[name], jnp.float32)
    for key, name in zip(kv, NAMES, strict=True):
        drawn[f"v_{name}"] = jax.random.uniform(key, SHAPES[name], jnp.float32, 0.005, 0.015)
    return drawn


def matmul(a, w):
    return jnp.dot(a, w, preferred_element_type=jnp.float32).astype(jnp.bfloat16)


def normed(h):
    wide = h.astype(jnp.float32)
    scale = lax.rsqrt(jnp.mean(wide**2, -1, keepdims=True) + 1e-6)
    return (wide * scale).astype(jnp.bfloat16)


def layer(h, w):
    a = normed(h)
    gate = jnp.dot(a, w["w_gate"], preferred_element_type=jnp.float32)
    up = jnp.dot(a, w["w_up"], preferred_element_type=jnp.float32)
    return h + matmul((jax.nn.silu(gate) * up).astype(jnp.bfloat16), w["w_down"])


def adamw(w, m, v, g):
    m = 0.9 * m + 0.1 * g
    v = 0.95 * v + 0.05 * g * g
    step = m * lax.rsqrt(v + 1e-8) + 0.1 * w
    return (w - 0.02 * step).astype(jnp.bfloat16), m, v


def clipped(gradients, sum_of_squares, count):
    factor = jnp.minimum(1.0, 0.5 * lax.rsqrt(sum_of_squares / count + 1e-30))
    return [g * factor for g in gradients]


def stack(weights, h):
    return lax.scan(lambda h, w: (layer(h, w), None), h, weights)[0]


def reference(x, dy, w_gate, w_up, w_down, m_w_gate, m_w_up, m_w_down, v_w_gate, v_w_up, v_w_down):
    weights = dict(zip(NAMES, (w_gate, w_up, w_down), strict=True))

    def take(so_far, sequence):
        h, by_y = sequence
        _, back = jax.vjp(lambda w: stack(w, h), weights)
        return jax.tree.map(lambda total, term: total + term.astype(jnp.float32), so_far, back(by_y)[0]), None

    none_yet = {name: jnp.zeros(w.shape, jnp.float32) for name, w in weights.items()}
    by_weights, _ = lax.scan(take, none_yet, (x, dy))
    gradients = [by_weights[name].astype(jnp.bfloat16).astype(jnp.float32) for name in NAMES]
    gradients = clipped(gradients, sum(jnp.sum(g * g) for g in gradients), sum(g.size for g in gradients))
    new = [
        adamw(w.astype(jnp.float32), m, v, g)
        for w, m, v, g in zip((w_gate, w_up, w_down), (m_w_gate, m_w_up, m_w_down), (v_w_gate, v_w_up, v_w_down), gradients, strict=True)
    ]
    return tuple(one[which] for which in range(3) for one in new)
```

```python
import functools
import jax, jax.numpy as jnp
from jax import lax
from jax.experimental import pallas as pl
from jax.experimental.pallas import tpu as pltpu

T, D, FF = 2048, 512, 8192
C = 512
NT = (((1,), (1,)), ((), ()))

def dot(a, b):
    return jnp.dot(a, b, preferred_element_type=jnp.float32)

def dot_nt(a, b):
    return lax.dot_general(a, b, NT, preferred_element_type=jnp.float32)

def norm_to(h_ref, a_ref):
    wide = h_ref[...].astype(jnp.float32)
    scale = lax.rsqrt(jnp.mean(wide * wide, -1, keepdims=True) + 1e-6)
    a_ref[...] = (wide * scale).astype(jnp.bfloat16)

def fwd_kernel(x, wg, wu, wd, h1, a_s, acc):
    k = pl.program_id(0)

    @pl.when(k == 0)
    def _():
        norm_to(x, a_s)
        acc[...] = jnp.zeros_like(acc)

    def chunk(c, _):
        rows = pl.ds(pl.multiple_of(c * C, C), C)
        a = a_s[rows, :]
        gate = dot(a, wg[0])
        up = dot(a, wu[0])
        act = (gate * jax.nn.sigmoid(gate) * up).astype(jnp.bfloat16)
        acc[rows, :] += dot(act, wd[0])
        return 0

    lax.fori_loop(0, T // C, chunk, 0)

    @pl.when(k == pl.num_programs(0) - 1)
    def _():
        h1[...] = x[...] + acc[...].astype(jnp.bfloat16)

def forward(x, wg, wu, wd, layer, F=512):
    return pl.pallas_call(
        fwd_kernel,
        grid=(FF // F,),
        in_specs=[
            pl.BlockSpec((T, D), lambda k: (0, 0)),
            pl.BlockSpec((1, D, F), lambda k: (layer, 0, k)),
            pl.BlockSpec((1, D, F), lambda k: (layer, 0, k)),
            pl.BlockSpec((1, F, D), lambda k: (layer, k, 0)),
        ],
        out_specs=pl.BlockSpec((T, D), lambda k: (0, 0)),
        out_shape=jax.ShapeDtypeStruct((T, D), jnp.bfloat16),
        scratch_shapes=[pltpu.VMEM((T, D), jnp.bfloat16), pltpu.VMEM((T, D), jnp.float32)],
        cost_estimate=pl.CostEstimate(flops=6 * T * D * FF, bytes_accessed=3 * D * FF * 2, transcendentals=0),
        compiler_params=pltpu.CompilerParams(vmem_limit_bytes=56 << 20, dimension_semantics=("arbitrary",)),
    )(x, wg, wu, wd)

MESH = pl.DeviceIdType.MESH
ORDERS = ((0, 1, 2), (1, 2, 0), (2, 0, 1))

def place():
    me = lax.axis_index("dp")
    return me, [me // bit % 2 for bit in (8, 4, 2, 1)]

def other(me, mask):
    for bit in (8, 4, 2, 1):
        if mask & bit:
            me = me + bit * (1 - 2 * (me // bit % 2))
    return me

def greet(masks):
    me, _ = place()
    barrier = pltpu.get_barrier_semaphore()
    for mask in masks:
        pl.semaphore_signal(barrier, inc=1, device_id={"dp": other(me, mask)}, device_id_type=MESH)
    pl.semaphore_wait(barrier, len(masks))

def rs_scratch(S):
    vm = lambda *lead: pltpu.VMEM(lead + (256, 512), jnp.bfloat16)
    per = [vm(2, 2, 2), vm(2, 2, 2), vm(2, 2), vm(2), vm()]
    return per * 3 + [pltpu.SemaphoreType.DMA((3, S)), pltpu.SemaphoreType.DMA((4, 3, S)), pltpu.SemaphoreType.DMA((4, 3, S))]
RS_REFS = 18

class Scatter:
    def __init__(self, g, refs, S):
        self.g, self.S, self.R = g, S, 256 // S
        self.buf = [refs[5 * p : 5 * p + 5] for p in range(3)]
        self.loc, self.snd, self.rcv = refs[15:18]
        self.me, self.at = place()

    def rows(self, s):
        return pl.ds(s * self.R, self.R)

    def copy(self, step, p, s):
        own = self.buf[p][0]
        rows = self.rows(s)
        if step == 0:
            src, bit = self.g[p].at[:, :, :, 1 - self.at[3], rows], 1
        else:
            order = ORDERS[p]
            index = [slice(None)] * 3
            for axis in order[: step - 1]:
                index[axis] = self.at[axis]
            index[order[step - 1]] = 1 - self.at[order[step - 1]]
            src, bit = own.at[(*index, rows)], 8 >> order[step - 1]
        into = self.buf[p][step + 1]
        dst = into.at[(slice(None),) * (len(into.shape) - 2) + (rows,)]
        return pltpu.make_async_remote_copy(
            src_ref=src, dst_ref=dst, send_sem=self.snd.at[step, p, s], recv_sem=self.rcv.at[step, p, s],
            device_id={"dp": other(self.me, bit)}, device_id_type=MESH)

    def local(self, p, s):
        rows = self.rows(s)
        return pltpu.make_async_copy(self.g[p].at[:, :, :, self.at[3], rows], self.buf[p][0].at[:, :, :, rows], self.loc.at[p, s])

    def summed(self, p, upto, index, rows):
        order = ORDERS[p]
        total = self.buf[p][0][(*index, rows, slice(None))].astype(jnp.float32)
        total += self.buf[p][1][(*index, rows, slice(None))].astype(jnp.float32)
        for n in range(1, upto):
            left = sorted(order[n:])
            total += self.buf[p][n + 1][(*[index[axis] for axis in left], rows, slice(None))].astype(jnp.float32)
        return total

    def start(self, s):
        for p in range(3):
            self.copy(0, p, s).start()
            self.local(p, s).start()

    def advance(self, step, s):
        for p in range(3):
            order = ORDERS[p]
            if step == 1:
                self.local(p, s).wait()
            self.copy(step - 1, p, s).wait_recv()
            free = order[step:]

            def block(i, _):
                index = [None] * 3
                for axis in order[: step - 1]:
                    index[axis] = self.at[axis]
                index[order[step - 1]] = 1 - self.at[order[step - 1]]
                n = i // max(1, self.R // 64)
                for axis in free:
                    index[axis] = n % 2
                    n = n // 2
                small = min(64, self.R)
                rows = pl.ds(pl.multiple_of(s * self.R + i % (self.R // small) * small, small), small)
                self.buf[p][0][(*index, rows, slice(None))] = self.summed(p, step, index, rows).astype(jnp.bfloat16)
                return 0

            lax.fori_loop(0, (1 << len(free)) * max(1, self.R // 64), block, 0)
            self.copy(step, p, s).start()

    def finish(self, s, outs):
        for p in range(3):
            self.copy(3, p, s).wait_recv()
            rows = self.rows(s)
            outs[p][rows, :] = self.summed(p, 4, self.at[:3], rows).astype(jnp.bfloat16)
        for step in range(4):
            for p in range(3):
                self.copy(step, p, s).wait_send()

def bwd_kernel(need_da, last, hosts, *refs):
    refs = list(refs)
    h, dh = refs[:2]
    wg, wu, wd = refs[2:4], refs[4:6], refs[6:8]
    refs = refs[8:]
    da_in = refs.pop(0) if need_da and last else None
    if hosts:
        g_in, refs = refs[:3], refs[3:]
    gg, gu, gd = refs[:3]
    refs = refs[3:]
    da_out = refs.pop(0) if need_da else None
    if hosts:
        summed, refs = refs[:3], refs[3:]
    a_s, aT, dhT, dg_s, du_s, act_s = refs[:6]
    refs = refs[6:]
    acc = refs.pop(0) if need_da else None
    da_sem = refs.pop(0) if need_da and last else None
    k = pl.program_id(0)
    if hosts:
        scatter = Scatter(g_in, refs, 1)

        @pl.when(k == 0)
        def _():
            greet((8, 4, 2, 1))
            scatter.start(0)

        for step, when in ((1, 2), (2, 5), (3, 7)):
            @pl.when(k == when)
            def _():
                scatter.advance(step, 0)

    @pl.when(k == 0)
    def _():
        norm_to(h, a_s)
        aT[...] = a_s[...].T
        dhT[...] = dh[...].T
        if need_da:
            if last:
                copy = pltpu.make_async_copy(da_in, acc, da_sem)
                copy.start()
                copy.wait()
            else:
                acc[...] = jnp.zeros_like(acc)

    def chunk(c, _):
        rows = pl.ds(pl.multiple_of(c * C, C), C)
        a = a_s[rows, :]
        dy = dh[rows, :]
        for b in range(2):
            cols = slice(b * 256, b * 256 + 256)
            gate = dot(a, wg[b][0])
            up = dot(a, wu[b][0])
            dact = dot_nt(dy, wd[b][0]).astype(jnp.bfloat16).astype(jnp.float32)
            s = jax.nn.sigmoid(gate)
            silu = gate * s
            act_s[rows, cols] = (silu * up).astype(jnp.bfloat16)
            du_s[rows, cols] = (dact * silu).astype(jnp.bfloat16)
            dg_s[rows, cols] = (dact * up * (s + silu * (1.0 - s))).astype(jnp.bfloat16)
        if need_da:
            t = acc[rows, :]
            for b in range(2):
                cols = slice(b * 256, b * 256 + 256)
                t += dot_nt(dg_s[rows, cols], wg[b][0]) + dot_nt(du_s[rows, cols], wu[b][0])
            acc[rows, :] = t
        return 0

    lax.fori_loop(0, T // C, chunk, 0)
    gg[...] = dot(aT[...], dg_s[...]).astype(jnp.bfloat16).reshape(16, 32, 512)
    gu[...] = dot(aT[...], du_s[...]).astype(jnp.bfloat16).reshape(16, 32, 512)
    gd[...] = dot(dhT[...], act_s[...]).T.astype(jnp.bfloat16).reshape(2, 256, 512)

    if need_da:
        @pl.when(k == pl.num_programs(0) - 1)
        def _():
            if not last:
                da_out[...] = acc[...]
            else:
                wide = h[...].astype(jnp.float32)
                scale = lax.rsqrt(jnp.mean(wide * wide, -1, keepdims=True) + 1e-6)
                da = acc[...].astype(jnp.bfloat16).astype(jnp.float32)
                along = jnp.mean(da * wide, -1, keepdims=True)
                da_out[...] = dh[...] + (da * scale - wide * (scale * scale * scale * along)).astype(jnp.bfloat16)

    if hosts:
        @pl.when(k == pl.num_programs(0) - 1)
        def _():
            scatter.finish(0, summed)

G = jax.ShapeDtypeStruct((16, 256, 512), jnp.bfloat16)
OWN = jax.ShapeDtypeStruct((256, 512), jnp.bfloat16)

def backward(h, dh, wg, wu, wd, layer, half, need_da, da=None, g=None, number=None):
    last = da is not None
    hosts = g is not None
    whole = pl.BlockSpec((T, D), lambda k: (0, 0), pipeline_mode=pl.Buffered(1))
    wide = [pl.BlockSpec((1, D, 256), lambda k, b=b: (layer, 0, (2 * k + b) * 2 + half)) for b in range(2)]
    tall = [pl.BlockSpec((1, 256, D), lambda k, b=b: (layer, (2 * k + b) * 2 + half, 0)) for b in range(2)]
    outs = [G, G, G]
    out_specs = [pl.BlockSpec((16, 32, 512), lambda k: (0, k, 0))] * 2 + [pl.BlockSpec((2, 256, 512), lambda k: (k, 0, 0))]
    scratch = [pltpu.VMEM((T, D), jnp.bfloat16), pltpu.VMEM((D, T), jnp.bfloat16), pltpu.VMEM((D, T), jnp.bfloat16)]
    scratch += [pltpu.VMEM((T, 512), jnp.bfloat16)] * 3
    args = [h, dh, wg, wg, wu, wu, wd, wd]
    in_specs = [whole, whole] + wide * 2 + tall
    if need_da:
        outs.append(jax.ShapeDtypeStruct((T, D), jnp.bfloat16 if last else jnp.float32))
        out_specs.append(whole)
        scratch.append(pltpu.VMEM((T, D), jnp.float32))
        if last:
            args.append(da)
            in_specs.append(pl.BlockSpec(memory_space=pl.ANY))
            scratch.append(pltpu.SemaphoreType.DMA)
    params = {}
    if hosts:
        args += [t.reshape(2, 2, 2, 2, 256, 512) for t in g]
        in_specs += [pl.BlockSpec(memory_space=pl.ANY)] * 3
        outs += [OWN] * 3
        out_specs += [pl.BlockSpec((256, 512), lambda k: (0, 0))] * 3
        scratch += rs_scratch(1)
        params = {"collective_id": number, "has_side_effects": True}
    out = pl.pallas_call(
        functools.partial(bwd_kernel, need_da, last, hosts),
        grid=(8,),
        in_specs=in_specs,
        out_specs=out_specs,
        out_shape=outs,
        scratch_shapes=scratch,
        cost_estimate=pl.CostEstimate(flops=(16 if need_da else 12) * T * D * FF // 2, bytes_accessed=3 * D * FF * 2, transcendentals=0),
        compiler_params=pltpu.CompilerParams(vmem_limit_bytes=62 << 20, dimension_semantics=("arbitrary",), **params),
    )(*args)
    return out[:3], (out[3] if need_da else None), (out[-3:] if hosts else None)

TAIL = 4

def tail_kernel(*refs):
    g_in, done, (a, b, c, total), refs = refs[:3], refs[3:12], refs[12:16], refs[16:]
    scatter = Scatter(g_in, refs[:RS_REFS], TAIL)
    parts, snd, rcv = refs[RS_REFS:]
    me, _ = place()
    greet(range(1, 16))
    for t in range(TAIL + 4):
        for step in range(4, -1, -1):
            s = t - step
            if 0 <= s < TAIL:
                if step == 0:
                    scatter.start(s)
                elif step < 4:
                    scatter.advance(step, s)
                else:
                    scatter.finish(s, (a, b, c))
    square = jnp.zeros((1, 512), jnp.float32)
    for ref in (*done, a, b, c):
        wide = ref[...].astype(jnp.float32)
        square += jnp.sum(wide * wide, 0, keepdims=True)
    square = square[:, :128] + square[:, 128:256] + square[:, 256:384] + square[:, 384:]
    parts[me] = jnp.broadcast_to(square, (8, 128))
    copies = [
        pltpu.make_async_remote_copy(
            src_ref=parts.at[me], dst_ref=parts.at[me], send_sem=snd.at[mask], recv_sem=rcv.at[mask],
            device_id={"dp": other(me, mask)}, device_id_type=MESH)
        for mask in range(1, 16)
    ]
    for copy in copies:
        copy.start()
    for copy in copies:
        copy.wait()
    whole = jnp.sum(parts[...], 0)
    total[...] = jnp.broadcast_to(jnp.sum(whole, 1, keepdims=True), (8, 128))

def tail(g, done):
    return pl.pallas_call(
        tail_kernel,
        in_specs=[pl.BlockSpec(memory_space=pl.ANY)] * 3 + [pl.BlockSpec(memory_space=pltpu.VMEM)] * 9,
        out_specs=[pl.BlockSpec(memory_space=pltpu.VMEM)] * 4,
        out_shape=[OWN] * 3 + [jax.ShapeDtypeStruct((8, 128), jnp.float32)],
        scratch_shapes=rs_scratch(TAIL) + [pltpu.VMEM((16, 8, 128), jnp.float32), pltpu.SemaphoreType.DMA((16,)), pltpu.SemaphoreType.DMA((16,))],
        compiler_params=pltpu.CompilerParams(vmem_limit_bytes=48 << 20, collective_id=4, has_side_effects=True),
    )(*[t.reshape(2, 2, 2, 2, 256, 512) for t in g], *done)

def update_kernel(me, total, *refs):
    g, (ws, ms, vs), outs = refs[:12], (refs[12:15], refs[15:18], refs[18:21]), refs[21:]
    factor = jnp.minimum(1.0, 0.5 * lax.rsqrt(total[0:1, 0:1] / (3 * 2 * D * FF) + 1e-30))
    k = pl.program_id(0)

    def one(i, at, grad):
        grad = grad.astype(jnp.float32) * factor
        m = 0.9 * ms[i][at] + 0.1 * grad
        v = 0.95 * vs[i][at] + 0.05 * grad * grad
        w = ws[i][at].astype(jnp.float32)
        outs[i][at] = (w - 0.02 * (m * lax.rsqrt(v + 1e-8) + 0.1 * w)).astype(jnp.bfloat16)
        outs[3 + i][at] = m
        outs[6 + i][at] = v

    for layer in range(2):
        for half in range(2):
            for i in range(2):
                for b in range(2):
                    grad = g[(layer * 2 + half) * 3 + i][:, b * 256 : b * 256 + 256]
                    one(i, (layer, slice(None), slice(b * 512 + half * 256, b * 512 + half * 256 + 256)), grad)

            @pl.when(k // 4 == half)
            def _():
                one(2, (layer,), g[(layer * 2 + half) * 3 + 2][...])

def update(me, total, g, w, m, v):
    wide = pl.BlockSpec((2, 32, 1024), lambda k, me: (0, 0, k))
    tall = pl.BlockSpec((2, 64, 512), lambda k, me: (0, k, 0))
    state = [wide, wide, tall]
    weights = [pl.BlockSpec((2, 32, 1024), lambda k, me: (0, me[0], k))] * 2 + [pl.BlockSpec((2, 64, 512), lambda k, me: (0, me[0] * 8 + k, 0))]
    grads = ([pl.BlockSpec((32, 512), lambda k, me: (k, 0))] * 2 + [pl.BlockSpec((64, 512), lambda k, me: (k % 4, 0))]) * 4
    shapes = [(2, 32, FF), (2, 32, FF), (2, 512, D)]
    return pl.pallas_call(
        update_kernel,
        grid_spec=pltpu.PrefetchScalarGridSpec(
            num_scalar_prefetch=1,
            grid=(8,),
            in_specs=[pl.BlockSpec((8, 128), lambda k, me: (0, 0))] + grads + weights + state + state,
            out_specs=state * 3,
        ),
        out_shape=[jax.ShapeDtypeStruct(s, t) for t in (jnp.bfloat16, jnp.float32, jnp.float32) for s in shapes],
        compiler_params=pltpu.CompilerParams(vmem_limit_bytes=48 << 20, dimension_semantics=("arbitrary",)),
    )(me.reshape(1), total, *g, *w, *m, *v)

def gather_kernel(*refs):
    own, full, (loc, snd, rcv, csnd, crcv) = refs[:3], refs[3:6], refs[6:]
    me, at = place()
    greet((8, 4, 2, 1))

    def block(p, layer, number):
        n = full[p].shape[1] // 16
        return full[p].at[layer, pl.ds(pl.multiple_of(number * n, n), n)]

    def send(p, layer, number, slot, bit, sems):
        src = own[p].at[layer] if number is me else block(p, layer, number)
        copy = pltpu.make_async_remote_copy(
            src_ref=src, dst_ref=block(p, layer, number), send_sem=sems[0].at[p, layer, slot], recv_sem=sems[1].at[p, layer, slot],
            device_id={"dp": other(me, bit)}, device_id_type=MESH)
        copy.start()
        sent.append(copy)

    def arrived(p, layer, number, slot, sems):
        pltpu.make_async_remote_copy(
            src_ref=block(p, layer, number), dst_ref=block(p, layer, number), send_sem=sems[0].at[p, layer, slot],
            recv_sem=sems[1].at[p, layer, slot], device_id={"dp": other(me, 1)}, device_id_type=MESH).wait_recv()

    sent = []
    ici, core = (snd, rcv), (csnd, crcv)
    bits = [[8 >> axis for axis in order] for order in ORDERS]
    each = [(p, layer) for layer in range(2) for p in range(3)]
    local = [pltpu.make_async_copy(own[p].at[layer], block(p, layer, me), loc.at[p, layer]) for p, layer in each]
    for step in range(3):
        for p, layer in each:
            send(p, layer, me, 1 << step, bits[p][step], ici)
    for p, layer in each:
        send(p, layer, me, 0, 1, core)
    for copy in local:
        copy.start()
    for step in range(3):
        for slot in range(1 << step, 2 << step):
            for p, layer in each:
                mask = sum(bits[p][i] for i in range(3) if slot >> i & 1)
                number = other(me, mask)
                arrived(p, layer, number, slot, ici)
                for later in range(step + 1, 3):
                    send(p, layer, number, slot | 1 << later, bits[p][later], ici)
                send(p, layer, number, slot, 1, core)
    for slot in range(8):
        for p, layer in each:
            mask = sum(bits[p][i] for i in range(3) if slot >> i & 1)
            arrived(p, layer, other(me, mask + 1), slot, core)
    for copy in local:
        copy.wait()
    for copy in sent:
        copy.wait_send()

def gather(new):
    sems = lambda n: pltpu.SemaphoreType.DMA((3, 2, n))
    return pl.pallas_call(
        gather_kernel,
        in_specs=[pl.BlockSpec(memory_space=pltpu.VMEM)] * 3,
        out_specs=[pl.BlockSpec(memory_space=pl.ANY)] * 3,
        out_shape=[jax.ShapeDtypeStruct((2, t.shape[1] * 16, t.shape[2]), t.dtype) for t in new],
        scratch_shapes=[pltpu.SemaphoreType.DMA((3, 2)), sems(8), sems(8), sems(8), sems(8)],
        compiler_params=pltpu.CompilerParams(vmem_limit_bytes=32 << 20, collective_id=5, has_side_effects=True),
    )(*new)

def solution(mesh):
    P = jax.sharding.PartitionSpec
    rows = P(None, "dp", None)

    def step(x, dy, *arrays):
        x, dy = x[0], dy[0]
        w, m, v = (arrays[i : i + 3] for i in (0, 3, 6))
        h1 = forward(x, *w, 0)
        g1a, da, _ = backward(h1, dy, *w, 1, 0, True)
        g1b, dh, s1a = backward(h1, dy, *w, 1, 1, True, da=da, g=g1a, number=1)
        g0a, _, s1b = backward(x, dh, *w, 0, 0, False, g=g1b, number=2)
        g0b, _, s0a = backward(x, dh, *w, 0, 1, False, g=g0a, number=3)
        *s0b, total = tail(g0b, [*s1a, *s1b, *s0a])
        new = update(lax.axis_index("dp"), total, [*s0a, *s0b, *s1a, *s1b], w, m, v)
        return (*gather(new[:3]), *new[3:])

    return jax.shard_map(
        step,
        mesh=mesh,
        in_specs=(P(("rep", "dp")),) * 2 + (P(),) * 3 + (rows,) * 6,
        out_specs=(P("rep"),) * 3 + (P("rep", "dp"),) * 6,
        check_vma=False,
    )
```

```python
import functools
import jax, jax.numpy as jnp
from jax import lax
from jax.experimental import pallas as pl
from jax.experimental.pallas import tpu as pltpu

T, D, FF = 2048, 512, 8192
C = 256
UNROLL = 4
CB = 512
NT = (((1,), (1,)), ((), ()))

def dot(a, b):
    return jnp.dot(a, b, preferred_element_type=jnp.float32)

def dot_nt(a, b):
    return lax.dot_general(a, b, NT, preferred_element_type=jnp.float32)

def by_rows(body):
    lax.fori_loop(0, T // 256, lambda c, _: (body(pl.ds(pl.multiple_of(c * 256, 256), 256)), 0)[1], 0)

def norm_to(h_ref, a_ref):
    def some(rows):
        wide = h_ref[rows, :].astype(jnp.float32)
        scale = lax.rsqrt(jnp.mean(wide * wide, -1, keepdims=True) + 1e-6)
        a_ref[rows, :] = (wide * scale).astype(jnp.bfloat16)

    by_rows(some)

def fwd_kernel(x, wg, wu, wd, h1, gates, ups, a_s, acc):
    k = pl.program_id(0)

    @pl.when(k == 0)
    def _():
        norm_to(x, a_s)
        acc[...] = jnp.zeros_like(acc)

    def chunk(c, _):
        rows = pl.ds(pl.multiple_of(c * C, C), C)
        a = a_s[rows, :]
        gate = dot(a, wg[0])
        up = dot(a, wu[0])
        gates[rows, :] = gate
        ups[rows, :] = up
        act = (gate * jax.nn.sigmoid(gate) * up).astype(jnp.bfloat16)
        acc[rows, :] += dot(act, wd[0])
        return 0

    lax.fori_loop(0, T // C, chunk, 0, unroll=UNROLL)

    @pl.when(k == pl.num_programs(0) - 1)
    def _():
        h1[...] = x[...] + acc[...].astype(jnp.bfloat16)

def forward(x, wg, wu, wd, layer, F=1024):
    one = pl.Buffered(1)
    return pl.pallas_call(
        fwd_kernel,
        grid=(FF // F,),
        in_specs=[
            pl.BlockSpec((T, D), lambda k: (0, 0), pipeline_mode=one),
            pl.BlockSpec((1, D, F), lambda k: (layer, 0, k)),
            pl.BlockSpec((1, D, F), lambda k: (layer, 0, k)),
            pl.BlockSpec((1, F, D), lambda k: (layer, k, 0)),
        ],
        out_specs=[pl.BlockSpec((T, D), lambda k: (0, 0))] + [pl.BlockSpec((T, F), lambda k: (0, k))] * 2,
        out_shape=[jax.ShapeDtypeStruct((T, D), jnp.bfloat16)] + [jax.ShapeDtypeStruct((T, FF), jnp.float32)] * 2,
        scratch_shapes=[pltpu.VMEM((T, D), jnp.bfloat16), pltpu.VMEM((T, D), jnp.float32)],
        cost_estimate=pl.CostEstimate(flops=6 * T * D * FF, bytes_accessed=3 * D * FF * 2, transcendentals=0),
        compiler_params=pltpu.CompilerParams(vmem_limit_bytes=60 << 20, dimension_semantics=("arbitrary",)),
    )(x, wg, wu, wd)

HOSTED = 2
SCHEDULE = ((0, 0, 0), (1, 0, 1), (1, 1, 0), (2, 1, 1), (4, 2, 0), (5, 2, 1), (6, 3, 0), (7, 3, 1))
MESH = pl.DeviceIdType.MESH
ORDERS = ((0, 1, 2), (1, 2, 0), (2, 0, 1))

def place():
    me = lax.axis_index("dp")
    return me, [me // bit % 2 for bit in (8, 4, 2, 1)]

def other(me, mask):
    for bit in (8, 4, 2, 1):
        if mask & bit:
            me = me + bit * (1 - 2 * (me // bit % 2))
    return me

def greet(masks):
    me, _ = place()
    barrier = pltpu.get_barrier_semaphore()
    for mask in masks:
        pl.semaphore_signal(barrier, inc=1, device_id={"dp": other(me, mask)}, device_id_type=MESH)
    pl.semaphore_wait(barrier, len(masks))

def rs_scratch(S):
    vm = lambda *lead: pltpu.VMEM(lead + (256, 512), jnp.bfloat16)
    per = [vm(2, 2, 2), vm(2, 2, 2), vm(2, 2), vm(2), vm()]
    return per * 3 + [pltpu.SemaphoreType.DMA((3, S)), pltpu.SemaphoreType.DMA((4, 3, S)), pltpu.SemaphoreType.DMA((4, 3, S))]
RS_REFS = 18

class Scatter:
    def __init__(self, g, refs, S):
        self.g, self.S, self.R = g, S, 256 // S
        self.buf = [refs[5 * p : 5 * p + 5] for p in range(3)]
        self.loc, self.snd, self.rcv = refs[15:18]
        self.me, self.at = place()

    def rows(self, s):
        return pl.ds(pl.multiple_of(s * self.R, self.R), self.R)

    def copy(self, step, p, s):
        own = self.buf[p][0]
        rows = self.rows(s)
        if step == 0:
            src, bit = self.g[p].at[:, :, :, 1 - self.at[3], rows], 1
        else:
            order = ORDERS[p]
            index = [slice(None)] * 3
            for axis in order[: step - 1]:
                index[axis] = self.at[axis]
            index[order[step - 1]] = 1 - self.at[order[step - 1]]
            src, bit = own.at[(*index, rows)], 8 >> order[step - 1]
        into = self.buf[p][step + 1]
        dst = into.at[(slice(None),) * (len(into.shape) - 2) + (rows,)]
        return pltpu.make_async_remote_copy(
            src_ref=src, dst_ref=dst, send_sem=self.snd.at[step, p, s], recv_sem=self.rcv.at[step, p, s],
            device_id={"dp": other(self.me, bit)}, device_id_type=MESH)

    def local(self, p, s):
        rows = self.rows(s)
        return pltpu.make_async_copy(self.g[p].at[:, :, :, self.at[3], rows], self.buf[p][0].at[:, :, :, rows], self.loc.at[p, s])

    def summed(self, p, upto, index, rows):
        order = ORDERS[p]
        total = self.buf[p][0][(*index, rows, slice(None))].astype(jnp.float32)
        total += self.buf[p][1][(*index, rows, slice(None))].astype(jnp.float32)
        for n in range(1, upto):
            left = sorted(order[n:])
            total += self.buf[p][n + 1][(*[index[axis] for axis in left], rows, slice(None))].astype(jnp.float32)
        return total

    def start(self, s):
        for p in range(3):
            self.copy(0, p, s).start()
            self.local(p, s).start()

    def advance(self, step, s):
        for p in range(3):
            order = ORDERS[p]
            if step == 1:
                self.local(p, s).wait()
            self.copy(step - 1, p, s).wait_recv()
            free = order[step:]

            def block(i, _):
                index = [None] * 3
                for axis in order[: step - 1]:
                    index[axis] = self.at[axis]
                index[order[step - 1]] = 1 - self.at[order[step - 1]]
                n = i // (self.R // 64)
                for axis in free:
                    index[axis] = n % 2
                    n = n // 2
                rows = pl.ds(pl.multiple_of(s * self.R + i % (self.R // 64) * 64, 64), 64)
                self.buf[p][0][(*index, rows, slice(None))] = self.summed(p, step, index, rows).astype(jnp.bfloat16)
                return 0

            trips = (1 << len(free)) * (self.R // 64)
            lax.fori_loop(0, trips, block, 0, unroll=min(2, trips))
            self.copy(step, p, s).start()

    def finish(self, s, outs):
        for p in range(3):
            self.copy(3, p, s).wait_recv()
            rows = self.rows(s)
            outs[p][rows, :] = self.summed(p, 4, self.at[:3], rows).astype(jnp.bfloat16)
        for step in range(4):
            for p in range(3):
                self.copy(step, p, s).wait_send()

def bwd_kernel(need_da, last, hosts, *refs):
    refs = list(refs)
    h, dh = refs[:2]
    wg, wu, wd = refs[2:4], refs[4:6], refs[6:8]
    refs = refs[8:]
    da_in = refs.pop(0) if need_da and last else None
    if hosts:
        g_in, refs = refs[:3], refs[3:]
    gg, gu, gd = refs[:3]
    refs = refs[3:]
    da_out = refs.pop(0) if need_da else None
    if hosts:
        summed, refs = refs[:3], refs[3:]
    a_s, aT, dhT = refs[:3]
    terms, sums, refs = (refs[3:6], refs[6:9]), refs[9:12], refs[12:]
    acc = refs.pop(0) if need_da else None
    da_sem = refs.pop(0) if need_da and last else None
    k = pl.program_id(0)
    if hosts:
        scatter = Scatter(g_in, refs, HOSTED)

        @pl.when(k == 0)
        def _():
            greet((8, 4, 2, 1))

        for when, step, s in SCHEDULE:
            @pl.when(k == when)
            def _():
                scatter.advance(step, s) if step else scatter.start(s)

    @pl.when(k == 0)
    def _():
        norm_to(h, a_s)

        def turn(rows):
            aT[:, rows] = a_s[rows, :].T
            dhT[:, rows] = dh[rows, :].T

        by_rows(turn)
        if need_da:
            if last:
                copy = pltpu.make_async_copy(da_in, acc, da_sem)
                copy.start()
                copy.wait()
            else:
                acc[...] = jnp.zeros_like(acc)

    def states(c, b):
        rows = slice(c * CB, c * CB + CB)
        cols = slice(b * 256, b * 256 + 256)
        dg_s, du_s, act_s = terms[c % 2]
        gate = dot(a_s[rows, :], wg[b][0]) if need_da else wg[b][rows, :]
        up = dot(a_s[rows, :], wu[b][0]) if need_da else wu[b][rows, :]
        dact = dot_nt(dh[rows, :], wd[b][0]).astype(jnp.bfloat16).astype(jnp.float32)
        s = jax.nn.sigmoid(gate)
        silu = gate * s
        act_s[:, cols] = (silu * up).astype(jnp.bfloat16)
        du_s[:, cols] = (dact * silu).astype(jnp.bfloat16)
        dg_s[:, cols] = (dact * up * (s + silu * (1.0 - s))).astype(jnp.bfloat16)

    def weights(c, i):
        left = dhT if i == 2 else aT
        new = dot(left[:, c * CB : c * CB + CB], terms[c % 2][i][...])
        if c:
            new += sums[i][...]
        if c < T // CB - 1:
            sums[i][...] = new
        elif i == 2:
            gd[...] = new.T.astype(jnp.bfloat16).reshape(2, 256, 512)
        else:
            (gg, gu)[i][...] = new.astype(jnp.bfloat16).reshape(16, 32, 512)

    for c in range(T // CB + 1):
        if c < T // CB:
            states(c, 0)
        if c:
            weights(c - 1, 0)
        if c < T // CB:
            states(c, 1)
        if c:
            weights(c - 1, 1)
            weights(c - 1, 2)
        if need_da and c < T // CB:
            rows = slice(c * CB, c * CB + CB)
            dg_s, du_s, _ = terms[c % 2]
            acc[rows, :] += sum(
                dot_nt(t[:, b * 256 : b * 256 + 256], w[b][0]) for b in range(2) for t, w in ((dg_s, wg), (du_s, wu))
            )

    if need_da:
        @pl.when(k == pl.num_programs(0) - 1)
        def _():
            if not last:
                da_out[...] = acc[...]
            else:
                def some(rows):
                    wide = h[rows, :].astype(jnp.float32)
                    scale = lax.rsqrt(jnp.mean(wide * wide, -1, keepdims=True) + 1e-6)
                    da = acc[rows, :].astype(jnp.bfloat16).astype(jnp.float32)
                    along = jnp.mean(da * wide, -1, keepdims=True)
                    da_out[rows, :] = dh[rows, :] + (da * scale - wide * (scale * scale * scale * along)).astype(jnp.bfloat16)

                by_rows(some)

    if hosts:
        @pl.when(k == pl.num_programs(0) - 1)
        def _():
            for s in range(HOSTED):
                scatter.finish(s, summed)

G = jax.ShapeDtypeStruct((16, 256, 512), jnp.bfloat16)
OWN = jax.ShapeDtypeStruct((256, 512), jnp.bfloat16)

def backward(h, dh, wg, wu, wd, layer, half, need_da, da=None, g=None, number=None):
    last = da is not None
    hosts = g is not None
    whole = pl.BlockSpec((T, D), lambda k: (0, 0), pipeline_mode=pl.Buffered(1))
    wide = [pl.BlockSpec((1, D, 256), lambda k, b=b: (layer, 0, (2 * k + b) * 2 + half)) for b in range(2)]
    tall = [pl.BlockSpec((1, 256, D), lambda k, b=b: (layer, (2 * k + b) * 2 + half, 0)) for b in range(2)]
    outs = [G, G, G]
    out_specs = [pl.BlockSpec((16, 32, 512), lambda k: (0, k, 0))] * 2 + [pl.BlockSpec((2, 256, 512), lambda k: (k, 0, 0))]
    scratch = [pltpu.VMEM((T, D), jnp.bfloat16), pltpu.VMEM((D, T), jnp.bfloat16), pltpu.VMEM((D, T), jnp.bfloat16)]
    scratch += [pltpu.VMEM((CB, 512), jnp.bfloat16)] * 6 + [pltpu.VMEM((512, 512), jnp.float32)] * 3
    args = [h, dh, wg, wg, wu, wu, wd, wd]
    in_specs = [whole, whole] + wide * 2 + tall
    if not need_da:
        in_specs[2:6] = [pl.BlockSpec((T, 256), lambda k, b=b: (0, (2 * k + b) * 2 + half)) for b in range(2)] * 2
    if need_da:
        outs.append(jax.ShapeDtypeStruct((T, D), jnp.bfloat16 if last else jnp.float32))
        out_specs.append(whole)
        scratch.append(pltpu.VMEM((T, D), jnp.float32))
        if last:
            args.append(da)
            in_specs.append(pl.BlockSpec(memory_space=pl.ANY))
            scratch.append(pltpu.SemaphoreType.DMA)
    params = {}
    if hosts:
        args += [t.reshape(2, 2, 2, 2, 256, 512) for t in g]
        in_specs += [pl.BlockSpec(memory_space=pl.ANY)] * 3
        outs += [OWN] * 3
        out_specs += [pl.BlockSpec((256, 512), lambda k: (0, 0))] * 3
        scratch += rs_scratch(HOSTED)
        params = {"collective_id": number, "has_side_effects": True}
    out = pl.pallas_call(
        functools.partial(bwd_kernel, need_da, last, hosts),
        grid=(8,),
        in_specs=in_specs,
        out_specs=out_specs,
        out_shape=outs,
        scratch_shapes=scratch,
        cost_estimate=pl.CostEstimate(flops=(16 if need_da else 12) * T * D * FF // 2, bytes_accessed=3 * D * FF * 2, transcendentals=0),
        compiler_params=pltpu.CompilerParams(vmem_limit_bytes=62 << 20, dimension_semantics=("arbitrary",), **params),
    )(*args)
    return out[:3], (out[3] if need_da else None), (out[-3:] if hosts else None)

TAIL = 4

def tail_kernel(*refs):
    g_in, done, (a, b, c, total), refs = refs[:3], refs[3:12], refs[12:16], refs[16:]
    scatter = Scatter(g_in, refs[:RS_REFS], TAIL)
    parts, snd, rcv = refs[RS_REFS:]
    me, _ = place()
    greet(range(1, 16))
    def each(act):
        lax.fori_loop(0, TAIL, lambda s, _: (act(s), 0)[1], 0)

    each(scatter.start)
    for step in (1, 2, 3):
        each(lambda s: scatter.advance(step, s))
    each(lambda s: scatter.finish(s, (a, b, c)))
    square = jnp.zeros((1, 512), jnp.float32)
    for ref in (*done, a, b, c):
        wide = ref[...].astype(jnp.float32)
        square += jnp.sum(wide * wide, 0, keepdims=True)
    square = square[:, :128] + square[:, 128:256] + square[:, 256:384] + square[:, 384:]
    parts[me] = jnp.broadcast_to(square, (8, 128))
    copies = [
        pltpu.make_async_remote_copy(
            src_ref=parts.at[me], dst_ref=parts.at[me], send_sem=snd.at[mask], recv_sem=rcv.at[mask],
            device_id={"dp": other(me, mask)}, device_id_type=MESH)
        for mask in range(1, 16)
    ]
    for copy in copies:
        copy.start()
    for copy in copies:
        copy.wait()
    whole = jnp.sum(parts[...], 0)
    total[...] = jnp.broadcast_to(jnp.sum(whole, 1, keepdims=True), (8, 128))

def tail(g, done):
    return pl.pallas_call(
        tail_kernel,
        in_specs=[pl.BlockSpec(memory_space=pl.ANY)] * 3 + [pl.BlockSpec(memory_space=pltpu.VMEM)] * 9,
        out_specs=[pl.BlockSpec(memory_space=pltpu.VMEM)] * 4,
        out_shape=[OWN] * 3 + [jax.ShapeDtypeStruct((8, 128), jnp.float32)],
        scratch_shapes=rs_scratch(TAIL) + [pltpu.VMEM((16, 8, 128), jnp.float32), pltpu.SemaphoreType.DMA((16,)), pltpu.SemaphoreType.DMA((16,))],
        compiler_params=pltpu.CompilerParams(vmem_limit_bytes=48 << 20, collective_id=4, has_side_effects=True),
    )(*[t.reshape(2, 2, 2, 2, 256, 512) for t in g], *done)

def update_kernel(me, total, *refs):
    g, (ws, ms, vs), outs = refs[:12], (refs[12:15], refs[15:18], refs[18:21]), refs[21:]
    factor = jnp.minimum(1.0, 0.5 * lax.rsqrt(total[0:1, 0:1] / (3 * 2 * D * FF) + 1e-30))
    k = pl.program_id(0)

    def one(i, at, grad):
        grad = grad.astype(jnp.float32) * factor
        m = 0.9 * ms[i][at] + 0.1 * grad
        v = 0.95 * vs[i][at] + 0.05 * grad * grad
        w = ws[i][at].astype(jnp.float32)
        outs[i][at] = (w - 0.02 * (m * lax.rsqrt(v + 1e-8) + 0.1 * w)).astype(jnp.bfloat16)
        outs[3 + i][at] = m
        outs[6 + i][at] = v

    for layer in range(2):
        for half in range(2):
            for i in range(2):
                for b in range(2):
                    grad = g[(layer * 2 + half) * 3 + i][:, b * 256 : b * 256 + 256]
                    one(i, (layer, slice(None), slice(b * 512 + half * 256, b * 512 + half * 256 + 256)), grad)

            @pl.when(k // 4 == half)
            def _():
                one(2, (layer,), g[(layer * 2 + half) * 3 + 2][...])

def update(me, total, g, w, m, v):
    wide = pl.BlockSpec((2, 32, 1024), lambda k, me: (0, 0, k))
    tall = pl.BlockSpec((2, 64, 512), lambda k, me: (0, k, 0))
    state = [wide, wide, tall]
    weights = [pl.BlockSpec((2, 32, 1024), lambda k, me: (0, me[0], k))] * 2 + [pl.BlockSpec((2, 64, 512), lambda k, me: (0, me[0] * 8 + k, 0))]
    grads = ([pl.BlockSpec((32, 512), lambda k, me: (k, 0))] * 2 + [pl.BlockSpec((64, 512), lambda k, me: (k % 4, 0))]) * 4
    shapes = [(2, 32, FF), (2, 32, FF), (2, 512, D)]
    return pl.pallas_call(
        update_kernel,
        grid_spec=pltpu.PrefetchScalarGridSpec(
            num_scalar_prefetch=1,
            grid=(8,),
            in_specs=[pl.BlockSpec((8, 128), lambda k, me: (0, 0))] + grads + weights + state + state,
            out_specs=state * 3,
        ),
        out_shape=[jax.ShapeDtypeStruct(s, t) for t in (jnp.bfloat16, jnp.float32, jnp.float32) for s in shapes],
        compiler_params=pltpu.CompilerParams(vmem_limit_bytes=48 << 20, dimension_semantics=("arbitrary",)),
    )(me.reshape(1), total, *g, *w, *m, *v)

def gather_kernel(*refs):
    own, full, (loc, snd, rcv, csnd, crcv) = refs[:3], refs[3:6], refs[6:]
    me, at = place()
    greet((8, 4, 2, 1))

    def block(p, layer, number):
        n = full[p].shape[1] // 16
        return full[p].at[layer, pl.ds(pl.multiple_of(number * n, n), n)]

    def send(p, layer, number, slot, bit, sems):
        src = own[p].at[layer] if number is me else block(p, layer, number)
        copy = pltpu.make_async_remote_copy(
            src_ref=src, dst_ref=block(p, layer, number), send_sem=sems[0].at[p, layer, slot], recv_sem=sems[1].at[p, layer, slot],
            device_id={"dp": other(me, bit)}, device_id_type=MESH)
        copy.start()
        sent.append(copy)

    def arrived(p, layer, number, slot, sems):
        pltpu.make_async_remote_copy(
            src_ref=block(p, layer, number), dst_ref=block(p, layer, number), send_sem=sems[0].at[p, layer, slot],
            recv_sem=sems[1].at[p, layer, slot], device_id={"dp": other(me, 1)}, device_id_type=MESH).wait_recv()

    sent = []
    ici, core = (snd, rcv), (csnd, crcv)
    bits = [[8 >> axis for axis in order] for order in ORDERS]
    each = [(p, layer) for layer in range(2) for p in range(3)]
    local = [pltpu.make_async_copy(own[p].at[layer], block(p, layer, me), loc.at[p, layer]) for p, layer in each]
    for step in range(3):
        for p, layer in each:
            send(p, layer, me, 1 << step, bits[p][step], ici)
    for p, layer in each:
        send(p, layer, me, 0, 1, core)
    for copy in local:
        copy.start()
    for step in range(3):
        for slot in range(1 << step, 2 << step):
            for p, layer in each:
                mask = sum(bits[p][i] for i in range(3) if slot >> i & 1)
                number = other(me, mask)
                arrived(p, layer, number, slot, ici)
                for later in range(step + 1, 3):
                    send(p, layer, number, slot | 1 << later, bits[p][later], ici)
                send(p, layer, number, slot, 1, core)
    for slot in range(8):
        for p, layer in each:
            mask = sum(bits[p][i] for i in range(3) if slot >> i & 1)
            arrived(p, layer, other(me, mask + 1), slot, core)
    for copy in local:
        copy.wait()
    for copy in sent:
        copy.wait_send()

def gather(new):
    sems = lambda n: pltpu.SemaphoreType.DMA((3, 2, n))
    return pl.pallas_call(
        gather_kernel,
        in_specs=[pl.BlockSpec(memory_space=pltpu.VMEM)] * 3,
        out_specs=[pl.BlockSpec(memory_space=pl.ANY)] * 3,
        out_shape=[jax.ShapeDtypeStruct((2, t.shape[1] * 16, t.shape[2]), t.dtype) for t in new],
        scratch_shapes=[pltpu.SemaphoreType.DMA((3, 2)), sems(8), sems(8), sems(8), sems(8)],
        compiler_params=pltpu.CompilerParams(vmem_limit_bytes=32 << 20, collective_id=5, has_side_effects=True),
    )(*new)

def solution(mesh):
    P = jax.sharding.PartitionSpec
    rows = P(None, "dp", None)

    def step(x, dy, *arrays):
        x, dy = x[0], dy[0]
        w, m, v = (arrays[i : i + 3] for i in (0, 3, 6))
        h1, *gates = forward(x, *w, 0)
        g1a, da, _ = backward(h1, dy, *w, 1, 0, True)
        g1b, dh, s1a = backward(h1, dy, *w, 1, 1, True, da=da, g=g1a, number=1)
        g0a, _, s1b = backward(x, dh, *gates, w[2], 0, 0, False, g=g1b, number=2)
        g0b, _, s0a = backward(x, dh, *gates, w[2], 0, 1, False, g=g0a, number=3)
        *s0b, total = tail(g0b, [*s1a, *s1b, *s0a])
        new = update(lax.axis_index("dp"), total, [*s0a, *s0b, *s1a, *s1b], w, m, v)
        return (*gather(new[:3]), *new[3:])

    return jax.shard_map(
        step,
        mesh=mesh,
        in_specs=(P(("rep", "dp")),) * 2 + (P(),) * 3 + (rows,) * 6,
        out_specs=(P("rep"),) * 3 + (P("rep", "dp"),) * 6,
        check_vma=False,
    )
```
